32 devices in a mesh: groups: 2 (over x), expert: 16 (over z, y, core).
Axes of the slice: x: 2, y: 2, z: 4, core: 2. Of those that a mesh axis runs over, the one named last changes fastest.
Arguments:
- tokens: bfloat16 [128, 6144], P(('groups', 'expert')), parts along dimension 0, may hold values from -64 to 64
- router_weight: bfloat16 [12288, 4], P('groups'), parts along dimension 0, may hold values from -1 to 1
- expert_ids: int32 [128, 2], P(('groups', 'expert')), parts along dimension 0, may hold values from 0 to 3, as said below
- slots: int32 [128, 2], P(('groups', 'expert')), parts along dimension 0, may hold values from 0 to 3, as said below
- gate_weight: bfloat16 [6144, 32768], P(None, 'expert'), may hold values from -0.078125 to 0.078125
- up_weight: bfloat16 [6144, 32768], P(None, 'expert'), may hold values from -0.078125 to 0.078125
- down_weight: bfloat16 [32768, 6144], P('expert'), may hold values from -0.0625 to 0.0625
Outputs:
- mixed_rows: bfloat16 [128, 6144], P(('groups', 'expert')), parts along dimension 0
- balance: float32 [2], P('groups'), parts along dimension 0
The draws below stay inside these ranges and needn't reach their ends.
There are 2 independent parts, one for each index of `groups`. The reference program is written for one: setup_inputs(seed, part) draws one part's arguments, and reference() takes and returns one part's arrays. A program takes and returns all parts, laid end to end along the dimension named above; an argument that names none is the same for every part. Nothing has to cross between parts.
Inputs may be any that keep to these rules, and one draw needn't show every extreme that they name: `expert_ids`: each row names two different experts; one expert, drawn from the seed, is named by every token. Within the rows of one device the slots of the assignments to one expert are distinct; on every device exactly 2 assignments of the expert that every token names have slots below 2, and no expert has more.
All inputs are finite; a program needn't handle non-finite values.
Results may differ from the reference program's by a relative error of at most 0.0058.
Values may be sent and summed in bfloat16 or wider, within the bound.
A program may use at most 128 MiB of HBM per device.

```python
import math
import jax
import jax.numpy as jnp
from jax import lax

D = 6144
FF_EXP = 8192
EXPERTS = 4
TOK_DEV = 4
CAP = 2
TOKENS = 64
FF_DEV = 2048
N_EXPERT = 16


def route_ids(key):
    heavy = jax.random.randint(jax.random.fold_in(key, 11), (), 0, EXPERTS)
    offset = jax.random.randint(jax.random.fold_in(key, 12), (TOKENS,), 0, EXPERTS - 1)
    second_pick = (heavy + 1 + offset) % EXPERTS
    flipped = jax.random.randint(jax.random.fold_in(key, 13), (TOKENS,), 0, 2)
    first_col = jnp.where(flipped == 1, second_pick, heavy)
    second_col = jnp.where(flipped == 1, heavy, second_pick)
    return jnp.stack([first_col, second_col], axis=1).astype(jnp.int32)


def router_draw(key):
    values = jax.random.normal(jax.random.fold_in(key, 21), (D, EXPERTS), jnp.float32) / math.sqrt(D)
    return jnp.clip(values, -6.0 / math.sqrt(D), 6.0 / math.sqrt(D))


def draw_expert_ids(key, part):
    return route_ids(key)


def draw_router_weight(key, part):
    return router_draw(key).astype(jnp.bfloat16)


def draw_slots(key, part):
    routing = route_ids(key)
    blocks = TOKENS // TOK_DEV
    named = jnp.sum((routing[:, :, None] == jnp.arange(EXPERTS, dtype=jnp.int32)).astype(jnp.int32), axis=1)
    named = named.reshape(blocks, TOK_DEV, EXPERTS)
    ranking = jnp.clip(jnp.cumsum(named, axis=1) - 1, 0, TOK_DEV - 1)
    scores = jax.random.randint(jax.random.fold_in(key, 14), (blocks, EXPERTS, TOK_DEV), 0, 1 << 20)
    scores = scores * TOK_DEV + jnp.arange(TOK_DEV, dtype=jnp.int32)
    orders = jnp.argsort(scores, axis=2, stable=True).astype(jnp.int32)
    slot_table = jnp.take_along_axis(orders, jnp.transpose(ranking, (0, 2, 1)), axis=2)
    slot_table = jnp.transpose(slot_table, (0, 2, 1)).reshape(TOKENS, EXPERTS)
    return jnp.take_along_axis(slot_table, routing, axis=1).astype(jnp.int32)


def draw_tokens(key, part):
    row_pos = jnp.arange(TOKENS, dtype=jnp.float32)
    rising = jnp.exp(math.log(3.0) * row_pos / TOKENS)[:, None]
    row_scale = rising * jnp.exp(jax.random.uniform(jax.random.fold_in(key, 31), (TOKENS, 1), jnp.float32, math.log(0.7), math.log(1.4)))
    values = jax.random.normal(jax.random.fold_in(key, 32), (TOKENS, D), jnp.float32) * row_scale
    return jnp.clip(values, -64.0, 64.0).astype(jnp.bfloat16)


def block_scale(rng, dims, split, low, high):
    factor_of, own = 1.0, jax.random.fold_in(rng, 6)
    for position, blocks in split:
        heights = jnp.exp(jax.random.uniform(jax.random.fold_in(own, position), (blocks,), jnp.float32, low / len(split), high / len(split)))
        factor_of = factor_of * jnp.repeat(heights, dims[position] // blocks).reshape([-1 if axis == position else 1 for axis in range(len(dims))])
    return factor_of


def centred(stream_key, shape, scale, reach, cuts=(), kind=jnp.bfloat16):
    entries = jax.random.normal(stream_key, shape, jnp.float32) * scale
    if len(cuts) > 0:
        entries = block_scale(stream_key, shape, cuts, -0.22, 0.18) * entries
    return jnp.clip(entries, min=-reach, max=reach).astype(kind)


def setup_inputs(seed: int = 0, part: int = 0) -> dict:
    key_of = jax.random.split(jax.random.key(seed), 8)
    part_keys = jax.random.split(jax.random.fold_in(key_of[7], part), 8)
    tokens = draw_tokens(jax.random.fold_in(jax.random.fold_in(key_of[7], part), 71), part)
    router_weight = draw_router_weight(jax.random.fold_in(jax.random.fold_in(key_of[7], part), 71), part)
    expert_ids = draw_expert_ids(jax.random.fold_in(jax.random.fold_in(key_of[7], part), 71), part)
    slots = draw_slots(jax.random.fold_in(jax.random.fold_in(key_of[7], part), 71), part)
    gate_weight = centred(key_of[4], (D, EXPERTS * FF_EXP), D ** -0.5, 0.078125, ((1, 16),))
    up_weight = centred(key_of[5], (D, EXPERTS * FF_EXP), D ** -0.5, 0.078125, ((1, 16),))
    down_weight = centred(key_of[6], (EXPERTS * FF_EXP, D), FF_EXP ** -0.5, 0.0625, ((0, 16),))
    return {"tokens": tokens, "router_weight": router_weight, "expert_ids": expert_ids, "slots": slots, "gate_weight": gate_weight, "up_weight": up_weight, "down_weight": down_weight}


def expert_output(slot_rows, gate_weight, up_weight, down_weight, expert):
    group_size = N_EXPERT // EXPERTS

    def add_part(total, part_index):
        column = (expert * FF_EXP + part_index * FF_DEV).astype(jnp.int32)
        gate_cols = lax.dynamic_slice_in_dim(gate_weight, column, FF_DEV, 1)
        up_cols = lax.dynamic_slice_in_dim(up_weight, column, FF_DEV, 1)
        down_rows = lax.dynamic_slice_in_dim(down_weight, column, FF_DEV, 0)
        gate_pre = jnp.dot(slot_rows.astype(jnp.float32), gate_cols.astype(jnp.float32), preferred_element_type=jnp.float32)
        up_pre = jnp.dot(slot_rows.astype(jnp.float32), up_cols.astype(jnp.float32), preferred_element_type=jnp.float32)
        hidden = (jax.nn.silu(gate_pre) * up_pre).astype(jnp.bfloat16)
        partial_value = jnp.dot(hidden.astype(jnp.float32), down_rows.astype(jnp.float32), preferred_element_type=jnp.float32).astype(jnp.bfloat16)
        return (total + partial_value.astype(jnp.float32), None)
    start = jnp.zeros((slot_rows.shape[0], D), jnp.float32)
    total, unused = lax.scan(add_part, start, jnp.arange(group_size, dtype=jnp.int32))
    return total

def reference(tokens, router_weight, expert_ids, slots, gate_weight, up_weight, down_weight):
    blocks = TOKENS // TOK_DEV
    logits = jnp.dot(tokens.astype(jnp.float32), router_weight.astype(jnp.float32), preferred_element_type=jnp.float32)
    router_probs = jax.nn.softmax(logits, axis=1)
    chosen = jnp.take_along_axis(logits, expert_ids, axis=1)
    top_logit = jnp.max(chosen, axis=1, keepdims=True)
    raised = jnp.exp(chosen - top_logit)
    gate_values = raised / jnp.sum(raised, axis=1, keepdims=True)
    kept_gates = jnp.where(slots < CAP, gate_values, 0.0)
    named_onehot = (expert_ids[:, :, None] == jnp.arange(EXPERTS, dtype=jnp.int32)).astype(jnp.float32)
    counts = jnp.sum(named_onehot, axis=(0, 1))
    prob_sums = jnp.sum(router_probs, axis=0)
    balance = (EXPERTS * jnp.sum(counts / (2.0 * TOKENS) * (prob_sums / TOKENS))).reshape(1)
    slot_match = (slots[:, :, None, None] == jnp.arange(CAP, dtype=jnp.int32)).astype(jnp.float32)
    slot_onehot = named_onehot[:, :, :, None] * slot_match
    dispatch_map = jnp.sum(slot_onehot, axis=1).reshape(blocks, TOK_DEV, EXPERTS, CAP)
    combine_map = jnp.sum(slot_onehot * kept_gates[:, :, None, None], axis=1).reshape(blocks, TOK_DEV, EXPERTS, CAP)
    token_blocks = tokens.astype(jnp.float32).reshape(blocks, TOK_DEV, D)
    buffer = jnp.einsum('btec,btd->ebcd', dispatch_map, token_blocks, precision=lax.Precision.HIGHEST).astype(jnp.bfloat16)
    outputs = jnp.stack([expert_output(buffer[expert].reshape(blocks * CAP, D), gate_weight, up_weight, down_weight, expert).reshape(blocks, CAP, D) for expert in range(EXPERTS)])
    mixed_rows = jnp.einsum('btec,ebcd->btd', combine_map, outputs, precision=lax.Precision.HIGHEST)
    return (mixed_rows.reshape(TOKENS, D).astype(jnp.bfloat16), balance)
```

```python
import functools

import jax
import jax.numpy as jnp
from jax import lax
from jax.experimental import pallas as pl
from jax.experimental.pallas import tpu as pltpu
from jax.sharding import PartitionSpec as P

EXPERTS = 4
CAP = 2
MESH = pl.DeviceIdType.MESH
F32 = jnp.float32
BF16 = jnp.bfloat16

K_STEPS = 6
W_SLOTS = 5
D_PARTS = 6
MAIN_PARTS = 5
TAIL_PARTS = 2


def each(low, high, body):
    if high - low <= 16:
        for index in range(low, high):
            body(index)
    else:

        def step(index, carry):
            body(index)
            return carry

        lax.fori_loop(low, high, step, 0)


def kernel(
    n,
    tok_hbm,
    rw_hbm,
    ids_hbm,
    slots_hbm,
    gate_hbm,
    up_hbm,
    down_hbm,
    out_ref,
    bal_hbm,
    tok_ref,
    rw_ref,
    ids_ref,
    slots_ref,
    bal_ref,
    gate_buf,
    up_buf,
    down_buf,
    send_x,
    x_buf,
    acc_g,
    acc_u,
    hid,
    part,
    pair,
    summed,
    back,
    tail,
    weights,
    stat_own,
    stat_in,
    stat_pair,
    gate_sem,
    up_sem,
    down_sem,
    xs_sem,
    xr_sem,
    fs_sem,
    fr_sem,
    ps_sem,
    pr_sem,
    bs_sem,
    br_sem,
    ts_sem,
    tr_sem,
    ss_sem,
    sr_sem,
    in_sem,
    out_sem,
):
    me = lax.axis_index("expert")
    core = lax.rem(me, 2)
    chip = me // 2
    chips = n // 2
    per_expert = chips // EXPERTS
    partner = me + 1 - 2 * core
    tok_rows, width = tok_ref.shape
    k_rows = width // K_STEPS
    d_cols = width // D_PARTS
    t_cols = d_cols // TAIL_PARTS
    t_base = MAIN_PARTS * d_cols

    def chip_at(offset):
        return lax.rem(chip + offset, chips)

    def same_core(offset):
        return {"expert": chip_at(offset) * 2 + core}

    def weight_copy(k, source, target, sem):
        slot = lax.rem(k, W_SLOTS)
        rows = pl.ds(k * k_rows, k_rows)
        return pltpu.make_async_copy(source.at[rows], target.at[slot], sem.at[slot])

    def gate_copy(k):
        return weight_copy(k, gate_hbm, gate_buf, gate_sem)

    def up_copy(k):
        return weight_copy(k, up_hbm, up_buf, up_sem)

    def down_copy(j):
        cols = pl.ds(pl.multiple_of(j * d_cols, 128), d_cols)
        return pltpu.make_async_copy(down_hbm.at[:, cols], down_buf.at[j], down_sem.at[j])

    def tail_copy(t):
        cols = pl.ds(t_base + t * t_cols, t_cols)
        return pltpu.make_async_copy(
            down_hbm.at[:, cols],
            down_buf.at[0, :, pl.ds(t * t_cols, t_cols)],
            down_sem.at[MAIN_PARTS + t],
        )

    inputs = [
        pltpu.make_async_copy(source, target, in_sem.at[i])
        for i, (source, target) in enumerate(
            (
                (tok_hbm, tok_ref),
                (ids_hbm, ids_ref),
                (slots_hbm, slots_ref),
                (rw_hbm, rw_ref),
            )
        )
    ]
    for copy in inputs:
        copy.start()
    gate_copy(0).start()
    barrier = pltpu.get_barrier_semaphore()
    each(
        1,
        n,
        lambda o: pl.semaphore_signal(
            barrier, inc=1, device_id={"expert": lax.rem(me + o, n)}, device_id_type=MESH
        ),
    )

    for copy in inputs:
        copy.wait()
    up_copy(0).start()
    for k in range(1, W_SLOTS):
        gate_copy(k).start()
        up_copy(k).start()

    tok = tok_ref[...].astype(F32)
    ids = [[ids_ref[k, t] for k in range(2)] for t in range(tok_rows)]
    cells = [
        [
            jnp.where(slots_ref[k, t] < CAP, ids_ref[k, t] * CAP + slots_ref[k, t], -1)
            for k in range(2)
        ]
        for t in range(tok_rows)
    ]
    slot_of = lax.broadcasted_iota(jnp.int32, (CAP, width), 0)
    for e in range(EXPERTS):
        rows = jnp.zeros((CAP, width), F32)
        for t in range(tok_rows):
            for k in range(2):
                hit = slot_of + e * CAP == cells[t][k]
                rows = jnp.where(hit, jnp.broadcast_to(tok[t : t + 1], (CAP, width)), rows)
        send_x[e] = rows.astype(BF16)

    pl.semaphore_wait(barrier, n - 1)

    def k_cols_of(a):
        return pl.ds(pl.multiple_of(a * k_rows, 128), k_rows)

    def x_send(a, offset):
        return pltpu.make_async_remote_copy(
            src_ref=send_x.at[chip_at(offset) // per_expert, :, k_cols_of(a)],
            dst_ref=x_buf.at[core * chips + chip, :, k_cols_of(a)],
            send_sem=xs_sem.at[a],
            recv_sem=xr_sem.at[a],
            device_id=same_core(offset),
            device_id_type=MESH,
        )

    def x_own(a):
        return pltpu.make_async_copy(
            send_x.at[chip // per_expert, :, k_cols_of(a)],
            x_buf.at[core * chips + chip, :, k_cols_of(a)],
            xr_sem.at[a],
        )

    def x_wait(a):
        half = x_buf.at[pl.ds(core * chips, chips), :, k_cols_of(a)]
        pltpu.make_async_copy(half, half, xr_sem.at[a]).wait()

    def x_forward(a):
        half = x_buf.at[pl.ds(core * chips, chips), :, k_cols_of(a)]
        return pltpu.make_async_remote_copy(
            src_ref=half,
            dst_ref=half,
            send_sem=fs_sem.at[a],
            recv_sem=fr_sem.at[a],
            device_id={"expert": partner},
            device_id_type=MESH,
        )

    for a in range(K_STEPS):
        each(1, chips, lambda o, a=a: x_send(a, o).start())
        x_own(a).start()

    lane = lax.broadcasted_iota(jnp.int32, (tok_rows, 128), 1)
    row = lax.broadcasted_iota(jnp.int32, (tok_rows, 128), 0)
    logits = jnp.zeros((tok_rows, 128), F32)
    for e in range(EXPERTS):
        dots = jnp.sum(tok * rw_ref[e : e + 1, :].astype(F32), axis=1, keepdims=True)
        logits = jnp.where(lane == e, dots, logits)
    real = lane < EXPERTS
    top = jnp.max(jnp.where(real, logits, -jnp.inf), axis=1, keepdims=True)
    raised = jnp.where(real, jnp.exp(jnp.where(real, logits - top, 0.0)), 0.0)
    probs = raised / jnp.sum(raised, axis=1, keepdims=True)

    def column(values):
        result = jnp.zeros((tok_rows, 128), jnp.int32)
        for t in range(tok_rows):
            result = jnp.where(row == t, values[t], result)
        return result

    chosen = []
    for k in range(2):
        named = lane == column([ids[t][k] for t in range(tok_rows)])
        chosen.append(jnp.sum(jnp.where(named, logits, 0.0), axis=1, keepdims=True))
    top_two = jnp.maximum(chosen[0], chosen[1])
    lifted = [jnp.exp(value - top_two) for value in chosen]
    mix = jnp.zeros((tok_rows, 128), F32)
    for k in range(2):
        cell = column([cells[t][k] for t in range(tok_rows)])
        gate = lifted[k] / (lifted[0] + lifted[1])
        mix = mix + jnp.where(lane == cell, gate, 0.0)
    weights[...] = mix
    counts = jnp.zeros((tok_rows, 128), F32)
    for t in range(tok_rows):
        for k in range(2):
            counts = counts + jnp.where(lane == ids[t][k], 1.0, 0.0)
    stat_own[...] = jnp.zeros((8, 128), F32)
    stat_own[0:1] = counts[0:1]
    stat_own[1:2] = jnp.sum(probs, axis=0, keepdims=True)

    def stat_send(offset):
        return pltpu.make_async_remote_copy(
            src_ref=stat_own,
            dst_ref=stat_in.at[chip],
            send_sem=ss_sem.at[0],
            recv_sem=sr_sem.at[0],
            device_id=same_core(offset),
            device_id_type=MESH,
        )

    def stat_swap():
        return pltpu.make_async_remote_copy(
            src_ref=stat_pair.at[0],
            dst_ref=stat_pair.at[1],
            send_sem=ss_sem.at[1],
            recv_sem=sr_sem.at[1],
            device_id={"expert": partner},
            device_id_type=MESH,
        )

    each(1, chips, lambda o: stat_send(o).start())
    stat_mine = pltpu.make_async_copy(stat_own, stat_in.at[chip], sr_sem.at[0])
    stat_mine.start()

    acc_g[...] = jnp.zeros(acc_g.shape, F32)
    acc_u[...] = jnp.zeros(acc_u.shape, F32)

    x_wait(0)
    x_forward(0).start()

    def k_step(k, carry):
        @pl.when(k + 1 < K_STEPS)
        def _():
            x_wait(k + 1)
            x_forward(k + 1).start()

        x_forward(k).wait_recv()
        slot = lax.rem(k, W_SLOTS)
        cols = pl.ds(pl.multiple_of(k * k_rows, 128), k_rows)
        x = x_buf[:, :, cols].reshape(n * CAP, k_rows)
        gate_copy(k).wait()
        acc_g[...] += jnp.dot(x, gate_buf[slot], preferred_element_type=F32)
        up_copy(k).wait()
        acc_u[...] += jnp.dot(x, up_buf[slot], preferred_element_type=F32)

        @pl.when(k + W_SLOTS < K_STEPS)
        def _():
            gate_copy(k + W_SLOTS).start()
            up_copy(k + W_SLOTS).start()

        @pl.when((k >= 1) & (k <= MAIN_PARTS))
        def _():
            down_copy(k - 1).start()

        return carry

    lax.fori_loop(0, K_STEPS, k_step, 0)

    hid[...] = (jax.nn.silu(acc_g[...]) * acc_u[...]).astype(BF16)

    pltpu.make_async_copy(stat_in, stat_in, sr_sem.at[0]).wait()
    stat_pair[0] = jnp.sum(stat_in[...], axis=0)
    stat_swap().start()

    def d_cols_of(j):
        return pl.ds(pl.multiple_of(j * d_cols, 128), d_cols)

    def pair_send(j):
        return pltpu.make_async_remote_copy(
            src_ref=part.at[pl.ds((1 - core) * chips, chips), :, d_cols_of(j)],
            dst_ref=pair.at[:, :, d_cols_of(j)],
            send_sem=ps_sem.at[j],
            recv_sem=pr_sem.at[j],
            device_id={"expert": partner},
            device_id_type=MESH,
        )

    def back_send(j, offset):
        return pltpu.make_async_remote_copy(
            src_ref=summed.at[chip_at(offset), :, d_cols_of(j)],
            dst_ref=back.at[chip, :, d_cols_of(j)],
            send_sem=bs_sem.at[j],
            recv_sem=br_sem.at[j],
            device_id=same_core(offset),
            device_id_type=MESH,
        )

    def back_own(j):
        return pltpu.make_async_copy(
            summed.at[chip, :, d_cols_of(j)], back.at[chip, :, d_cols_of(j)], br_sem.at[j]
        )

    def add_pair(j):
        pair_send(j).wait_recv()
        mine = part[pl.ds(core * chips, chips), :, d_cols_of(j)].astype(F32)
        summed[:, :, d_cols_of(j)] = (mine + pair[:, :, d_cols_of(j)].astype(F32)).astype(BF16)
        each(1, chips, lambda o: back_send(j, o).start())
        back_own(j).start()

    def d_step(j, carry):
        down_copy(j).wait()
        value = jnp.dot(hid[...], down_buf[j], preferred_element_type=F32)
        part[:, :, d_cols_of(j)] = value.astype(BF16).reshape(n, CAP, d_cols)
        pair_send(j).start()

        @pl.when(j == 0)
        def _():
            for t in range(TAIL_PARTS):
                tail_copy(t).start()

        @pl.when(j > 0)
        def _():
            add_pair(j - 1)

        return carry

    def device_at(offset):
        return lax.rem(me + offset, n)

    def row_of(device):
        return lax.rem(device, 2) * chips + device // 2

    def tail_cols(t):
        return pl.ds(t_base + t * t_cols, t_cols)

    def tail_send(t, offset):
        return pltpu.make_async_remote_copy(
            src_ref=part.at[row_of(device_at(offset)), :, tail_cols(t)],
            dst_ref=tail.at[t, me],
            send_sem=ts_sem.at[t],
            recv_sem=tr_sem.at[t],
            device_id={"expert": device_at(offset)},
            device_id_type=MESH,
        )

    def tail_own(t):
        return pltpu.make_async_copy(
            part.at[row_of(me), :, tail_cols(t)], tail.at[t, me], tr_sem.at[t]
        )

    lax.fori_loop(0, MAIN_PARTS, d_step, 0)
    for t in range(TAIL_PARTS):
        tail_copy(t).wait()
        weight = down_buf[0, :, t * t_cols : (t + 1) * t_cols]
        value = jnp.dot(hid[...], weight, preferred_element_type=F32)
        part[:, :, tail_cols(t)] = value.astype(BF16).reshape(n, CAP, t_cols)
        each(1, n, lambda o, t=t: tail_send(t, o).start())
        tail_own(t).start()
        if t == 0:
            add_pair(MAIN_PARTS - 1)

    stat_swap().wait_recv()
    total = stat_pair[0] + stat_pair[1]
    tokens_in_all = float(tok_rows * n)
    terms = (total[0:1] / (2.0 * tokens_in_all)) * (total[1:2] / tokens_in_all)
    bal_ref[...] = jnp.broadcast_to(EXPERTS * jnp.sum(terms, axis=1, keepdims=True), (1, 128))
    bal_out = pltpu.make_async_copy(bal_ref, bal_hbm, out_sem.at[0])
    bal_out.start()
    stat_swap().wait_send()
    each(1, chips, lambda o: stat_send(o).wait_send())
    for a in range(K_STEPS):
        each(1, chips, lambda o, a=a: x_send(a, o).wait_send())
        x_forward(a).wait_send()

    mix_of = [weights[:, c : c + 1] for c in range(EXPERTS * CAP)]

    def mix_rows(blocks, cols, per_block):
        count = per_expert * per_block
        mixed = jnp.zeros((tok_rows, cols.size), F32)
        for e in range(EXPERTS):
            value = jnp.sum(blocks[e * count : (e + 1) * count].astype(F32), axis=0)
            for c in range(CAP):
                mixed = mixed + mix_of[e * CAP + c] * value[c : c + 1]
        out_ref[:, cols] = mixed.astype(BF16)

    for j in range(MAIN_PARTS):
        pair_send(j).wait_send()
        each(1, chips, lambda o, j=j: back_send(j, o).wait_send())
        cols = pl.ds(j * d_cols, d_cols)
        whole = back.at[:, :, cols]
        pltpu.make_async_copy(whole, whole, br_sem.at[j]).wait()
        mix_rows(back[:, :, cols], cols, 1)
    for t in range(TAIL_PARTS):
        pltpu.make_async_copy(tail.at[t], tail.at[t], tr_sem.at[t]).wait()
        mix_rows(tail[t], tail_cols(t), 2)
        each(1, n, lambda o, t=t: tail_send(t, o).wait_send())
    bal_out.wait()


def local(n, tokens, router_weight, expert_ids, slots, gate_weight, up_weight, down_weight):
    tok_rows, width = tokens.shape
    hidden = gate_weight.shape[1]
    chips = n // 2
    k_rows, d_cols = width // K_STEPS, width // D_PARTS
    anywhere = pl.BlockSpec(memory_space=pl.ANY)
    dma = pltpu.SemaphoreType.DMA
    mixed_rows, balance = pl.pallas_call(
        functools.partial(kernel, n),
        out_shape=(
            pltpu.VMEM((tok_rows, width), BF16),
            jax.ShapeDtypeStruct((1, 128), F32),
        ),
        in_specs=[anywhere] * 7,
        out_specs=(pl.BlockSpec(memory_space=pltpu.VMEM), anywhere),
        scratch_shapes=[
            pltpu.VMEM((tok_rows, width), BF16),
            pltpu.VMEM((EXPERTS, width), BF16),
            pltpu.SMEM((2, tok_rows), jnp.int32),
            pltpu.SMEM((2, tok_rows), jnp.int32),
            pltpu.VMEM((1, 128), F32),
            pltpu.VMEM((W_SLOTS, k_rows, hidden), BF16),
            pltpu.VMEM((W_SLOTS, k_rows, hidden), BF16),
            pltpu.VMEM((MAIN_PARTS, hidden, d_cols), BF16),
            pltpu.VMEM((EXPERTS, CAP, width), BF16),
            pltpu.VMEM((n, CAP, width), BF16),
            pltpu.VMEM((n * CAP, hidden), F32),
            pltpu.VMEM((n * CAP, hidden), F32),
            pltpu.VMEM((n * CAP, hidden), BF16),
            pltpu.VMEM((n, CAP, width), BF16),
            pltpu.VMEM((chips, CAP, width), BF16),
            pltpu.VMEM((chips, CAP, width), BF16),
            pltpu.VMEM((chips, CAP, width), BF16),
            pltpu.VMEM((TAIL_PARTS, n, CAP, d_cols // TAIL_PARTS), BF16),
            pltpu.VMEM((tok_rows, 128), F32),
            pltpu.VMEM((8, 128), F32),
            pltpu.VMEM((chips, 8, 128), F32),
            pltpu.VMEM((2, 8, 128), F32),
            dma((W_SLOTS,)),
            dma((W_SLOTS,)),
            dma((MAIN_PARTS + TAIL_PARTS,)),
            dma((K_STEPS,)),
            dma((K_STEPS,)),
            dma((K_STEPS,)),
            dma((K_STEPS,)),
            dma((MAIN_PARTS,)),
            dma((MAIN_PARTS,)),
            dma((MAIN_PARTS,)),
            dma((MAIN_PARTS,)),
            dma((TAIL_PARTS,)),
            dma((TAIL_PARTS,)),
            dma((2,)),
            dma((2,)),
            dma((4,)),
            dma((1,)),
        ],
        compiler_params=pltpu.CompilerParams(
            collective_id=0, has_side_effects=True, vmem_limit_bytes=66_800_000
        ),
    )(
        tokens,
        router_weight.T,
        expert_ids.T,
        slots.T,
        gate_weight,
        up_weight,
        down_weight,
    )
    return mixed_rows, balance[0, :1]


def solution(mesh):
    in_specs = (
        P(("groups", "expert"), None),
        P("groups", None),
        P(("groups", "expert"), None),
        P(("groups", "expert"), None),
        P(None, "expert"),
        P(None, "expert"),
        P("expert", None),
    )
    out_specs = (P(("groups", "expert"), None), P("groups"))
    return jax.shard_map(
        functools.partial(local, mesh.shape["expert"]),
        mesh=mesh,
        in_specs=in_specs,
        out_specs=out_specs,
        check_vma=False,
    )
```

```python
import functools

import jax
import jax.numpy as jnp
from jax import lax
from jax.experimental import pallas as pl
from jax.experimental.pallas import tpu as pltpu
from jax.sharding import PartitionSpec as P

EXPERTS = 4
CAP = 2
MESH = pl.DeviceIdType.MESH
F32 = jnp.float32
BF16 = jnp.bfloat16

K_STEPS = 6
W_SLOTS = 5
D_PARTS = 6
MAIN_PARTS = 5
TAIL_PARTS = 2


def each(low, high, body):
    if high - low <= 16:
        for index in range(low, high):
            body(index)
    else:

        def step(index, carry):
            body(index)
            return carry

        lax.fori_loop(low, high, step, 0)


def kernel(
    n,
    tok_hbm,
    rw_hbm,
    ids_hbm,
    slots_hbm,
    gate_hbm,
    up_hbm,
    down_hbm,
    out_ref,
    bal_hbm,
    tok_ref,
    rw_ref,
    ids_ref,
    slots_ref,
    bal_ref,
    gate_buf,
    up_buf,
    down_buf,
    send_x,
    x_buf,
    acc_g,
    acc_u,
    hid,
    part,
    pair,
    summed,
    back,
    tail_out,
    tail,
    weights,
    stat_own,
    stat_in,
    stat_pair,
    gate_sem,
    up_sem,
    down_sem,
    xs_sem,
    xr_sem,
    fs_sem,
    fr_sem,
    ps_sem,
    pr_sem,
    bs_sem,
    br_sem,
    ts_sem,
    tr_sem,
    ss_sem,
    sr_sem,
    in_sem,
    out_sem,
):
    me = lax.axis_index("expert")
    core = lax.rem(me, 2)
    chip = me // 2
    chips = n // 2
    per_expert = chips // EXPERTS
    partner = me + 1 - 2 * core
    tok_rows, width = tok_ref.shape
    k_rows = width // K_STEPS
    d_cols = width // D_PARTS
    t_cols = d_cols // TAIL_PARTS
    t_base = MAIN_PARTS * d_cols

    def chip_at(offset):
        return lax.rem(chip + offset, chips)

    def same_core(offset):
        return {"expert": chip_at(offset) * 2 + core}

    def weight_copy(k, source, target, sem):
        slot = lax.rem(k, W_SLOTS)
        rows = pl.ds(k * k_rows, k_rows)
        return pltpu.make_async_copy(source.at[rows], target.at[slot], sem.at[slot])

    def gate_copy(k):
        return weight_copy(k, gate_hbm, gate_buf, gate_sem)

    def up_copy(k):
        return weight_copy(k, up_hbm, up_buf, up_sem)

    def down_copy(j):
        cols = pl.ds(pl.multiple_of(j * d_cols, 128), d_cols)
        return pltpu.make_async_copy(down_hbm.at[:, cols], down_buf.at[j], down_sem.at[j])

    def tail_copy(t):
        cols = pl.ds(t_base + t * t_cols, t_cols)
        return pltpu.make_async_copy(
            down_hbm.at[:, cols],
            down_buf.at[0, :, pl.ds(t * t_cols, t_cols)],
            down_sem.at[MAIN_PARTS + t],
        )

    inputs = [
        pltpu.make_async_copy(source, target, in_sem.at[i])
        for i, (source, target) in enumerate(
            (
                (tok_hbm, tok_ref),
                (ids_hbm, ids_ref),
                (slots_hbm, slots_ref),
                (rw_hbm, rw_ref),
            )
        )
    ]
    for copy in inputs:
        copy.start()
    gate_copy(0).start()
    barrier = pltpu.get_barrier_semaphore()
    each(
        1,
        n,
        lambda o: pl.semaphore_signal(
            barrier, inc=1, device_id={"expert": lax.rem(me + o, n)}, device_id_type=MESH
        ),
    )

    for copy in inputs:
        copy.wait()
    up_copy(0).start()
    for k in range(1, W_SLOTS):
        gate_copy(k).start()
        up_copy(k).start()

    tok = tok_ref[...].astype(F32)
    ids = [[ids_ref[k, t] for k in range(2)] for t in range(tok_rows)]
    cells = [
        [
            jnp.where(slots_ref[k, t] < CAP, ids_ref[k, t] * CAP + slots_ref[k, t], -1)
            for k in range(2)
        ]
        for t in range(tok_rows)
    ]
    slot_of = lax.broadcasted_iota(jnp.int32, (CAP, width), 0)
    for e in range(EXPERTS):
        rows = jnp.zeros((CAP, width), F32)
        for t in range(tok_rows):
            for k in range(2):
                hit = slot_of + e * CAP == cells[t][k]
                rows = jnp.where(hit, jnp.broadcast_to(tok[t : t + 1], (CAP, width)), rows)
        send_x[e] = rows.astype(BF16)

    pl.semaphore_wait(barrier, n - 1)

    def k_cols_of(a):
        return pl.ds(pl.multiple_of(a * k_rows, 128), k_rows)

    def x_send(a, offset):
        return pltpu.make_async_remote_copy(
            src_ref=send_x.at[chip_at(offset) // per_expert, :, k_cols_of(a)],
            dst_ref=x_buf.at[core * chips + chip, :, k_cols_of(a)],
            send_sem=xs_sem.at[a],
            recv_sem=xr_sem.at[a],
            device_id=same_core(offset),
            device_id_type=MESH,
        )

    def x_own(a):
        return pltpu.make_async_copy(
            send_x.at[chip // per_expert, :, k_cols_of(a)],
            x_buf.at[core * chips + chip, :, k_cols_of(a)],
            xr_sem.at[a],
        )

    def x_wait(a):
        half = x_buf.at[pl.ds(core * chips, chips), :, k_cols_of(a)]
        pltpu.make_async_copy(half, half, xr_sem.at[a]).wait()

    def x_forward(a):
        half = x_buf.at[pl.ds(core * chips, chips), :, k_cols_of(a)]
        return pltpu.make_async_remote_copy(
            src_ref=half,
            dst_ref=half,
            send_sem=fs_sem.at[a],
            recv_sem=fr_sem.at[a],
            device_id={"expert": partner},
            device_id_type=MESH,
        )

    for a in range(K_STEPS):
        each(1, chips, lambda o, a=a: x_send(a, o).start())
        x_own(a).start()

    lane = lax.broadcasted_iota(jnp.int32, (tok_rows, 128), 1)
    row = lax.broadcasted_iota(jnp.int32, (tok_rows, 128), 0)
    logits = jnp.zeros((tok_rows, 128), F32)
    for e in range(EXPERTS):
        dots = jnp.sum(tok * rw_ref[e : e + 1, :].astype(F32), axis=1, keepdims=True)
        logits = jnp.where(lane == e, dots, logits)
    real = lane < EXPERTS
    top = jnp.max(jnp.where(real, logits, -jnp.inf), axis=1, keepdims=True)
    raised = jnp.where(real, jnp.exp(jnp.where(real, logits - top, 0.0)), 0.0)
    probs = raised / jnp.sum(raised, axis=1, keepdims=True)

    def column(values):
        result = jnp.zeros((tok_rows, 128), jnp.int32)
        for t in range(tok_rows):
            result = jnp.where(row == t, values[t], result)
        return result

    chosen = []
    for k in range(2):
        named = lane == column([ids[t][k] for t in range(tok_rows)])
        chosen.append(jnp.sum(jnp.where(named, logits, 0.0), axis=1, keepdims=True))
    top_two = jnp.maximum(chosen[0], chosen[1])
    lifted = [jnp.exp(value - top_two) for value in chosen]
    mix = jnp.zeros((tok_rows, 128), F32)
    for k in range(2):
        cell = column([cells[t][k] for t in range(tok_rows)])
        gate = lifted[k] / (lifted[0] + lifted[1])
        mix = mix + jnp.where(lane == cell, gate, 0.0)
    weights[...] = mix
    counts = jnp.zeros((tok_rows, 128), F32)
    for t in range(tok_rows):
        for k in range(2):
            counts = counts + jnp.where(lane == ids[t][k], 1.0, 0.0)
    stat_own[...] = jnp.zeros((8, 128), F32)
    stat_own[0:1] = counts[0:1]
    stat_own[1:2] = jnp.sum(probs, axis=0, keepdims=True)

    def stat_send(offset):
        return pltpu.make_async_remote_copy(
            src_ref=stat_own,
            dst_ref=stat_in.at[chip],
            send_sem=ss_sem.at[0],
            recv_sem=sr_sem.at[0],
            device_id=same_core(offset),
            device_id_type=MESH,
        )

    def stat_swap():
        return pltpu.make_async_remote_copy(
            src_ref=stat_pair.at[0],
            dst_ref=stat_pair.at[1],
            send_sem=ss_sem.at[1],
            recv_sem=sr_sem.at[1],
            device_id={"expert": partner},
            device_id_type=MESH,
        )

    each(1, chips, lambda o: stat_send(o).start())
    stat_mine = pltpu.make_async_copy(stat_own, stat_in.at[chip], sr_sem.at[0])
    stat_mine.start()

    acc_g[...] = jnp.zeros(acc_g.shape, F32)
    acc_u[...] = jnp.zeros(acc_u.shape, F32)

    x_wait(0)
    x_forward(0).start()

    def k_step(k, carry):
        @pl.when(k + 1 < K_STEPS)
        def _():
            x_wait(k + 1)
            x_forward(k + 1).start()

        x_forward(k).wait_recv()
        slot = lax.rem(k, W_SLOTS)
        cols = pl.ds(pl.multiple_of(k * k_rows, 128), k_rows)
        x = x_buf[:, :, cols].reshape(n * CAP, k_rows)
        gate_copy(k).wait()
        acc_g[...] += jnp.dot(x, gate_buf[slot], preferred_element_type=F32)
        up_copy(k).wait()
        acc_u[...] += jnp.dot(x, up_buf[slot], preferred_element_type=F32)

        @pl.when(k + W_SLOTS < K_STEPS)
        def _():
            gate_copy(k + W_SLOTS).start()
            up_copy(k + W_SLOTS).start()

        @pl.when((k >= 1) & (k <= MAIN_PARTS))
        def _():
            down_copy(k - 1).start()

        return carry

    lax.fori_loop(0, K_STEPS, k_step, 0)

    hid[...] = (jax.nn.silu(acc_g[...]) * acc_u[...]).astype(BF16)

    pltpu.make_async_copy(stat_in, stat_in, sr_sem.at[0]).wait()
    stat_pair[0] = jnp.sum(stat_in[...], axis=0)
    stat_swap().start()

    def d_cols_of(j):
        return pl.ds(pl.multiple_of(j * d_cols, 128), d_cols)

    def pair_send(j):
        return pltpu.make_async_remote_copy(
            src_ref=part.at[1 - core, :, d_cols_of(j)],
            dst_ref=pair.at[:, d_cols_of(j)],
            send_sem=ps_sem.at[j],
            recv_sem=pr_sem.at[j],
            device_id={"expert": partner},
            device_id_type=MESH,
        )

    def back_send(j, offset):
        return pltpu.make_async_remote_copy(
            src_ref=summed.at[chip_at(offset), :, d_cols_of(j)],
            dst_ref=back.at[chip, :, d_cols_of(j)],
            send_sem=bs_sem.at[j],
            recv_sem=br_sem.at[j],
            device_id=same_core(offset),
            device_id_type=MESH,
        )

    def back_own(j):
        return pltpu.make_async_copy(
            summed.at[chip, :, d_cols_of(j)], back.at[chip, :, d_cols_of(j)], br_sem.at[j]
        )

    def add_pair(j):
        pair_send(j).wait_recv()
        mine = part[core, :, d_cols_of(j)].astype(F32)
        both = (mine + pair[:, d_cols_of(j)].astype(F32)).astype(BF16)
        summed[:, :, d_cols_of(j)] = both.reshape(chips, CAP, d_cols)
        each(1, chips, lambda o: back_send(j, o).start())
        back_own(j).start()

    def d_step(j, carry):
        down_copy(j).wait()
        value = jnp.dot(hid[...], down_buf[j], preferred_element_type=F32)
        part[:, :, d_cols_of(j)] = value.astype(BF16).reshape(2, chips * CAP, d_cols)
        pair_send(j).start()

        @pl.when(j == 0)
        def _():
            for t in range(TAIL_PARTS):
                tail_copy(t).start()

        @pl.when(j > 0)
        def _():
            add_pair(j - 1)

        return carry

    def device_at(offset):
        return lax.rem(me + offset, n)

    def row_of(device):
        return lax.rem(device, 2) * chips + device // 2

    def tail_cols(t):
        return pl.ds(t_base + t * t_cols, t_cols)

    def tail_send(t, offset):
        return pltpu.make_async_remote_copy(
            src_ref=tail_out.at[t, row_of(device_at(offset))],
            dst_ref=tail.at[t, me],
            send_sem=ts_sem.at[t],
            recv_sem=tr_sem.at[t],
            device_id={"expert": device_at(offset)},
            device_id_type=MESH,
        )

    def tail_own(t):
        return pltpu.make_async_copy(
            tail_out.at[t, row_of(me)], tail.at[t, me], tr_sem.at[t]
        )

    lax.fori_loop(0, MAIN_PARTS, d_step, 0)
    for t in range(TAIL_PARTS):
        tail_copy(t).wait()
        weight = down_buf[0, :, t * t_cols : (t + 1) * t_cols]
        value = jnp.dot(hid[...], weight, preferred_element_type=F32)
        tail_out[t] = value.astype(BF16).reshape(n, CAP, t_cols)
        each(1, n, lambda o, t=t: tail_send(t, o).start())
        tail_own(t).start()
        if t == 0:
            add_pair(MAIN_PARTS - 1)

    stat_swap().wait_recv()
    total = stat_pair[0] + stat_pair[1]
    tokens_in_all = float(tok_rows * n)
    terms = (total[0:1] / (2.0 * tokens_in_all)) * (total[1:2] / tokens_in_all)
    bal_ref[...] = jnp.broadcast_to(EXPERTS * jnp.sum(terms, axis=1, keepdims=True), (1, 128))
    bal_out = pltpu.make_async_copy(bal_ref, bal_hbm, out_sem.at[0])
    bal_out.start()
    stat_swap().wait_send()
    each(1, chips, lambda o: stat_send(o).wait_send())
    for a in range(K_STEPS):
        each(1, chips, lambda o, a=a: x_send(a, o).wait_send())
        x_forward(a).wait_send()

    mix_of = [weights[:, c : c + 1] for c in range(EXPERTS * CAP)]

    def mix_rows(blocks, cols, per_block):
        count = per_expert * per_block
        mixed = jnp.zeros((tok_rows, cols.size), F32)
        for e in range(EXPERTS):
            value = jnp.sum(blocks[e * count : (e + 1) * count].astype(F32), axis=0)
            for c in range(CAP):
                mixed = mixed + mix_of[e * CAP + c] * value[c : c + 1]
        out_ref[:, cols] = mixed.astype(BF16)

    for j in range(MAIN_PARTS):
        pair_send(j).wait_send()
        each(1, chips, lambda o, j=j: back_send(j, o).wait_send())
        cols = pl.ds(j * d_cols, d_cols)
        whole = back.at[:, :, cols]
        pltpu.make_async_copy(whole, whole, br_sem.at[j]).wait()
        mix_rows(back[:, :, cols], cols, 1)
    bal_out.wait()
    for t in range(TAIL_PARTS):
        each(1, n, lambda o, t=t: tail_send(t, o).wait_send())
    for t in range(TAIL_PARTS):
        pltpu.make_async_copy(tail.at[t], tail.at[t], tr_sem.at[t]).wait()
        mix_rows(tail[t], tail_cols(t), 2)


def local(n, tokens, router_weight, expert_ids, slots, gate_weight, up_weight, down_weight):
    tok_rows, width = tokens.shape
    hidden = gate_weight.shape[1]
    chips = n // 2
    k_rows, d_cols = width // K_STEPS, width // D_PARTS
    anywhere = pl.BlockSpec(memory_space=pl.ANY)
    dma = pltpu.SemaphoreType.DMA
    mixed_rows, balance = pl.pallas_call(
        functools.partial(kernel, n),
        out_shape=(
            pltpu.VMEM((tok_rows, width), BF16),
            jax.ShapeDtypeStruct((1, 128), F32),
        ),
        in_specs=[anywhere] * 7,
        out_specs=(pl.BlockSpec(memory_space=pltpu.VMEM), anywhere),
        scratch_shapes=[
            pltpu.VMEM((tok_rows, width), BF16),
            pltpu.VMEM((EXPERTS, width), BF16),
            pltpu.SMEM((2, tok_rows), jnp.int32),
            pltpu.SMEM((2, tok_rows), jnp.int32),
            pltpu.VMEM((1, 128), F32),
            pltpu.VMEM((W_SLOTS, k_rows, hidden), BF16),
            pltpu.VMEM((W_SLOTS, k_rows, hidden), BF16),
            pltpu.VMEM((MAIN_PARTS, hidden, d_cols), BF16),
            pltpu.VMEM((EXPERTS, CAP, width), BF16),
            pltpu.VMEM((n, CAP, width), BF16),
            pltpu.VMEM((n * CAP, hidden), F32),
            pltpu.VMEM((n * CAP, hidden), F32),
            pltpu.VMEM((n * CAP, hidden), BF16),
            pltpu.VMEM((2, chips * CAP, width), BF16),
            pltpu.VMEM((chips * CAP, width), BF16),
            pltpu.VMEM((chips, CAP, width), BF16),
            pltpu.VMEM((chips, CAP, width), BF16),
            pltpu.VMEM((TAIL_PARTS, n, CAP, d_cols // TAIL_PARTS), BF16),
            pltpu.VMEM((TAIL_PARTS, n, CAP, d_cols // TAIL_PARTS), BF16),
            pltpu.VMEM((tok_rows, 128), F32),
            pltpu.VMEM((8, 128), F32),
            pltpu.VMEM((chips, 8, 128), F32),
            pltpu.VMEM((2, 8, 128), F32),
            dma((W_SLOTS,)),
            dma((W_SLOTS,)),
            dma((MAIN_PARTS + TAIL_PARTS,)),
            dma((K_STEPS,)),
            dma((K_STEPS,)),
            dma((K_STEPS,)),
            dma((K_STEPS,)),
            dma((MAIN_PARTS,)),
            dma((MAIN_PARTS,)),
            dma((MAIN_PARTS,)),
            dma((MAIN_PARTS,)),
            dma((TAIL_PARTS,)),
            dma((TAIL_PARTS,)),
            dma((2,)),
            dma((2,)),
            dma((4,)),
            dma((1,)),
        ],
        compiler_params=pltpu.CompilerParams(
            collective_id=0, has_side_effects=True, vmem_limit_bytes=66_800_000
        ),
    )(
        tokens,
        router_weight.T,
        expert_ids.T,
        slots.T,
        gate_weight,
        up_weight,
        down_weight,
    )
    return mixed_rows, balance[0, :1]


def solution(mesh):
    in_specs = (
        P(("groups", "expert"), None),
        P("groups", None),
        P(("groups", "expert"), None),
        P(("groups", "expert"), None),
        P(None, "expert"),
        P(None, "expert"),
        P("expert", None),
    )
    out_specs = (P(("groups", "expert"), None), P("groups"))
    return jax.shard_map(
        functools.partial(local, mesh.shape["expert"]),
        mesh=mesh,
        in_specs=in_specs,
        out_specs=out_specs,
        check_vma=False,
    )
```

```python
import functools

import jax
import jax.numpy as jnp
from jax import lax
from jax.experimental import pallas as pl
from jax.experimental.pallas import tpu as pltpu
from jax.sharding import PartitionSpec as P

EXPERTS = 4
CAP = 2
MESH = pl.DeviceIdType.MESH
F32 = jnp.float32
BF16 = jnp.bfloat16

K_STEPS = 6
W_SLOTS = 5
D_PARTS = 6
MAIN_PARTS = 5
TAIL_PARTS = 2


def each(low, high, body):
    if high - low <= 16:
        for index in range(low, high):
            body(index)
    else:

        def step(index, carry):
            body(index)
            return carry

        lax.fori_loop(low, high, step, 0)


def kernel(
    n,
    tok_hbm,
    rw_hbm,
    ids_hbm,
    slots_hbm,
    gate_hbm,
    up_hbm,
    down_hbm,
    out_ref,
    bal_ref,
    tok_ref,
    rw_ref,
    ids_ref,
    slots_ref,
    gate_buf,
    up_buf,
    down_buf,
    send_x,
    x_buf,
    acc_g,
    acc_u,
    hid,
    part,
    pair,
    summed,
    back,
    tail_out,
    tail,
    weights,
    stat_own,
    stat_in,
    stat_pair,
    gate_sem,
    up_sem,
    down_sem,
    xs_sem,
    xr_sem,
    fs_sem,
    fr_sem,
    ps_sem,
    pr_sem,
    bs_sem,
    br_sem,
    ts_sem,
    tr_sem,
    ss_sem,
    sr_sem,
    in_sem,
):
    me = lax.axis_index("expert")
    core = lax.rem(me, 2)
    chip = me // 2
    chips = n // 2
    per_expert = chips // EXPERTS
    partner = me + 1 - 2 * core
    tok_rows, width = tok_ref.shape
    k_rows = width // K_STEPS
    d_cols = width // D_PARTS
    t_cols = d_cols // TAIL_PARTS
    t_base = MAIN_PARTS * d_cols

    def chip_at(offset):
        return lax.rem(chip + offset, chips)

    def same_core(offset):
        return {"expert": chip_at(offset) * 2 + core}

    def weight_copy(k, source, target, sem):
        slot = lax.rem(k, W_SLOTS)
        rows = pl.ds(k * k_rows, k_rows)
        return pltpu.make_async_copy(source.at[rows], target.at[slot], sem.at[slot])

    def gate_copy(k):
        return weight_copy(k, gate_hbm, gate_buf, gate_sem)

    def up_copy(k):
        return weight_copy(k, up_hbm, up_buf, up_sem)

    def down_copy(j):
        cols = pl.ds(pl.multiple_of(j * d_cols, 128), d_cols)
        return pltpu.make_async_copy(down_hbm.at[:, cols], down_buf.at[j], down_sem.at[j])

    def tail_copy(t):
        cols = pl.ds(t_base + t * t_cols, t_cols)
        return pltpu.make_async_copy(
            down_hbm.at[:, cols],
            down_buf.at[0, :, pl.ds(t * t_cols, t_cols)],
            down_sem.at[MAIN_PARTS + t],
        )

    inputs = [
        pltpu.make_async_copy(source, target, in_sem.at[i])
        for i, (source, target) in enumerate(
            (
                (tok_hbm, tok_ref),
                (ids_hbm, ids_ref),
                (slots_hbm, slots_ref),
                (rw_hbm, rw_ref),
            )
        )
    ]
    for copy in inputs:
        copy.start()
    gate_copy(0).start()
    barrier = pltpu.get_barrier_semaphore()
    each(
        1,
        n,
        lambda o: pl.semaphore_signal(
            barrier, inc=1, device_id={"expert": lax.rem(me + o, n)}, device_id_type=MESH
        ),
    )

    for copy in inputs:
        copy.wait()
    up_copy(0).start()
    for k in range(1, W_SLOTS):
        gate_copy(k).start()
        up_copy(k).start()

    tok = tok_ref[...].astype(F32)
    ids = [[ids_ref[k, t] for k in range(2)] for t in range(tok_rows)]
    cells = [
        [
            jnp.where(slots_ref[k, t] < CAP, ids_ref[k, t] * CAP + slots_ref[k, t], -1)
            for k in range(2)
        ]
        for t in range(tok_rows)
    ]
    slot_of = lax.broadcasted_iota(jnp.int32, (CAP, width), 0)
    for e in range(EXPERTS):
        rows = jnp.zeros((CAP, width), F32)
        for t in range(tok_rows):
            for k in range(2):
                hit = slot_of + e * CAP == cells[t][k]
                rows = jnp.where(hit, jnp.broadcast_to(tok[t : t + 1], (CAP, width)), rows)
        send_x[e] = rows.astype(BF16)

    pl.semaphore_wait(barrier, n - 1)

    def k_cols_of(a):
        return pl.ds(pl.multiple_of(a * k_rows, 128), k_rows)

    def x_send(a, offset):
        return pltpu.make_async_remote_copy(
            src_ref=send_x.at[chip_at(offset) // per_expert, :, k_cols_of(a)],
            dst_ref=x_buf.at[core * chips + chip, :, k_cols_of(a)],
            send_sem=xs_sem.at[a],
            recv_sem=xr_sem.at[a],
            device_id=same_core(offset),
            device_id_type=MESH,
        )

    def x_own(a):
        return pltpu.make_async_copy(
            send_x.at[chip // per_expert, :, k_cols_of(a)],
            x_buf.at[core * chips + chip, :, k_cols_of(a)],
            xr_sem.at[a],
        )

    def x_wait(a):
        half = x_buf.at[pl.ds(core * chips, chips), :, k_cols_of(a)]
        pltpu.make_async_copy(half, half, xr_sem.at[a]).wait()

    def x_forward(a):
        half = x_buf.at[pl.ds(core * chips, chips), :, k_cols_of(a)]
        return pltpu.make_async_remote_copy(
            src_ref=half,
            dst_ref=half,
            send_sem=fs_sem.at[a],
            recv_sem=fr_sem.at[a],
            device_id={"expert": partner},
            device_id_type=MESH,
        )

    for a in range(K_STEPS):
        each(1, chips, lambda o, a=a: x_send(a, o).start())
        x_own(a).start()

    lane = lax.broadcasted_iota(jnp.int32, (tok_rows, 128), 1)
    row = lax.broadcasted_iota(jnp.int32, (tok_rows, 128), 0)
    logits = jnp.zeros((tok_rows, 128), F32)
    for e in range(EXPERTS):
        dots = jnp.sum(tok * rw_ref[e : e + 1, :].astype(F32), axis=1, keepdims=True)
        logits = jnp.where(lane == e, dots, logits)
    real = lane < EXPERTS
    top = jnp.max(jnp.where(real, logits, -jnp.inf), axis=1, keepdims=True)
    raised = jnp.where(real, jnp.exp(jnp.where(real, logits - top, 0.0)), 0.0)
    probs = raised / jnp.sum(raised, axis=1, keepdims=True)

    def column(values):
        result = jnp.zeros((tok_rows, 128), jnp.int32)
        for t in range(tok_rows):
            result = jnp.where(row == t, values[t], result)
        return result

    chosen = []
    for k in range(2):
        named = lane == column([ids[t][k] for t in range(tok_rows)])
        chosen.append(jnp.sum(jnp.where(named, logits, 0.0), axis=1, keepdims=True))
    top_two = jnp.maximum(chosen[0], chosen[1])
    lifted = [jnp.exp(value - top_two) for value in chosen]
    mix = jnp.zeros((tok_rows, 128), F32)
    for k in range(2):
        cell = column([cells[t][k] for t in range(tok_rows)])
        gate = lifted[k] / (lifted[0] + lifted[1])
        mix = mix + jnp.where(lane == cell, gate, 0.0)
    weights[...] = mix
    counts = jnp.zeros((tok_rows, 128), F32)
    for t in range(tok_rows):
        for k in range(2):
            counts = counts + jnp.where(lane == ids[t][k], 1.0, 0.0)
    stat_own[...] = jnp.zeros((8, 128), F32)
    stat_own[0:1] = counts[0:1]
    stat_own[1:2] = jnp.sum(probs, axis=0, keepdims=True)

    def stat_send(offset):
        return pltpu.make_async_remote_copy(
            src_ref=stat_own,
            dst_ref=stat_in.at[chip],
            send_sem=ss_sem.at[0],
            recv_sem=sr_sem.at[0],
            device_id=same_core(offset),
            device_id_type=MESH,
        )

    def stat_swap():
        return pltpu.make_async_remote_copy(
            src_ref=stat_pair.at[0],
            dst_ref=stat_pair.at[1],
            send_sem=ss_sem.at[1],
            recv_sem=sr_sem.at[1],
            device_id={"expert": partner},
            device_id_type=MESH,
        )

    each(1, chips, lambda o: stat_send(o).start())
    stat_mine = pltpu.make_async_copy(stat_own, stat_in.at[chip], sr_sem.at[0])
    stat_mine.start()

    acc_g[...] = jnp.zeros(acc_g.shape, F32)
    acc_u[...] = jnp.zeros(acc_u.shape, F32)

    x_wait(0)
    x_forward(0).start()

    def k_step(k, carry):
        @pl.when(k + 1 < K_STEPS)
        def _():
            x_wait(k + 1)
            x_forward(k + 1).start()

        x_forward(k).wait_recv()
        slot = lax.rem(k, W_SLOTS)
        cols = pl.ds(pl.multiple_of(k * k_rows, 128), k_rows)
        x = x_buf[:, :, cols].reshape(n * CAP, k_rows)
        gate_copy(k).wait()
        acc_g[...] += jnp.dot(x, gate_buf[slot], preferred_element_type=F32)
        up_copy(k).wait()
        acc_u[...] += jnp.dot(x, up_buf[slot], preferred_element_type=F32)

        @pl.when(k + W_SLOTS < K_STEPS)
        def _():
            gate_copy(k + W_SLOTS).start()
            up_copy(k + W_SLOTS).start()

        @pl.when((k >= 1) & (k <= MAIN_PARTS))
        def _():
            down_copy(k - 1).start()

        return carry

    lax.fori_loop(0, K_STEPS, k_step, 0)

    hid[...] = (jax.nn.silu(acc_g[...]) * acc_u[...]).astype(BF16)

    pltpu.make_async_copy(stat_in, stat_in, sr_sem.at[0]).wait()
    stat_pair[0] = jnp.sum(stat_in[...], axis=0)
    stat_swap().start()

    def d_cols_of(j):
        return pl.ds(pl.multiple_of(j * d_cols, 128), d_cols)

    def pair_send(j):
        return pltpu.make_async_remote_copy(
            src_ref=part.at[1 - core, :, d_cols_of(j)],
            dst_ref=pair.at[:, d_cols_of(j)],
            send_sem=ps_sem.at[j],
            recv_sem=pr_sem.at[j],
            device_id={"expert": partner},
            device_id_type=MESH,
        )

    def back_send(j, offset):
        return pltpu.make_async_remote_copy(
            src_ref=summed.at[chip_at(offset), :, d_cols_of(j)],
            dst_ref=back.at[chip, :, d_cols_of(j)],
            send_sem=bs_sem.at[j],
            recv_sem=br_sem.at[j],
            device_id=same_core(offset),
            device_id_type=MESH,
        )

    def back_own(j):
        return pltpu.make_async_copy(
            summed.at[chip, :, d_cols_of(j)], back.at[chip, :, d_cols_of(j)], br_sem.at[j]
        )

    def add_pair(j):
        pair_send(j).wait_recv()
        mine = part[core, :, d_cols_of(j)].astype(F32)
        both = (mine + pair[:, d_cols_of(j)].astype(F32)).astype(BF16)
        summed[:, :, d_cols_of(j)] = both.reshape(chips, CAP, d_cols)
        each(1, chips, lambda o: back_send(j, o).start())
        back_own(j).start()

    def d_step(j, carry):
        down_copy(j).wait()
        value = jnp.dot(hid[...], down_buf[j], preferred_element_type=F32)
        part[:, :, d_cols_of(j)] = value.astype(BF16).reshape(2, chips * CAP, d_cols)
        pair_send(j).start()

        @pl.when(j == 0)
        def _():
            for t in range(TAIL_PARTS):
                tail_copy(t).start()

        @pl.when(j > 0)
        def _():
            add_pair(j - 1)

        return carry

    def device_at(offset):
        return lax.rem(me + offset, n)

    def row_of(device):
        return lax.rem(device, 2) * chips + device // 2

    def tail_cols(t):
        return pl.ds(t_base + t * t_cols, t_cols)

    def tail_send(t, offset):
        return pltpu.make_async_remote_copy(
            src_ref=tail_out.at[t, row_of(device_at(offset))],
            dst_ref=tail.at[t, me],
            send_sem=ts_sem.at[t],
            recv_sem=tr_sem.at[t],
            device_id={"expert": device_at(offset)},
            device_id_type=MESH,
        )

    def tail_own(t):
        return pltpu.make_async_copy(
            tail_out.at[t, row_of(me)], tail.at[t, me], tr_sem.at[t]
        )

    lax.fori_loop(0, MAIN_PARTS, d_step, 0)
    for t in range(TAIL_PARTS):
        tail_copy(t).wait()
        weight = down_buf[0, :, t * t_cols : (t + 1) * t_cols]
        value = jnp.dot(hid[...], weight, preferred_element_type=F32)
        tail_out[t] = value.astype(BF16).reshape(n, CAP, t_cols)
        each(1, n, lambda o, t=t: tail_send(t, o).start())
        tail_own(t).start()
        if t == 0:
            add_pair(MAIN_PARTS - 1)

    stat_swap().wait_recv()
    total = stat_pair[0] + stat_pair[1]
    tokens_in_all = float(tok_rows * n)
    terms = (total[0:1] / (2.0 * tokens_in_all)) * (total[1:2] / tokens_in_all)
    bal_ref[...] = jnp.broadcast_to(EXPERTS * jnp.sum(terms, axis=1, keepdims=True), (1, 128))
    stat_swap().wait_send()
    each(1, chips, lambda o: stat_send(o).wait_send())
    for a in range(K_STEPS):
        each(1, chips, lambda o, a=a: x_send(a, o).wait_send())
        x_forward(a).wait_send()

    mix_of = [weights[:, c : c + 1] for c in range(EXPERTS * CAP)]

    def mix_rows(blocks, cols, per_block):
        count = per_expert * per_block
        mixed = jnp.zeros((tok_rows, cols.size), F32)
        for e in range(EXPERTS):
            value = jnp.sum(blocks[e * count : (e + 1) * count].astype(F32), axis=0)
            for c in range(CAP):
                mixed = mixed + mix_of[e * CAP + c] * value[c : c + 1]
        out_ref[:, cols] = mixed.astype(BF16)

    for j in range(MAIN_PARTS):
        pair_send(j).wait_send()
        each(1, chips, lambda o, j=j: back_send(j, o).wait_send())
        cols = pl.ds(j * d_cols, d_cols)
        whole = back.at[:, :, cols]
        pltpu.make_async_copy(whole, whole, br_sem.at[j]).wait()
        mix_rows(back[:, :, cols], cols, 1)
    for t in range(TAIL_PARTS):
        each(1, n, lambda o, t=t: tail_send(t, o).wait_send())
    for t in range(TAIL_PARTS):
        pltpu.make_async_copy(tail.at[t], tail.at[t], tr_sem.at[t]).wait()
        mix_rows(tail[t], tail_cols(t), 2)


def store(mixed_ref, bal_ref, mixed_hbm, bal_hbm, sem):
    copies = (
        pltpu.make_async_copy(mixed_ref, mixed_hbm, sem.at[0]),
        pltpu.make_async_copy(bal_ref, bal_hbm, sem.at[1]),
    )
    for copy in copies:
        copy.start()
    for copy in copies:
        copy.wait()


def local(n, tokens, router_weight, expert_ids, slots, gate_weight, up_weight, down_weight):
    tok_rows, width = tokens.shape
    hidden = gate_weight.shape[1]
    chips = n // 2
    k_rows, d_cols = width // K_STEPS, width // D_PARTS
    anywhere = pl.BlockSpec(memory_space=pl.ANY)
    dma = pltpu.SemaphoreType.DMA
    mixed_rows, balance = pl.pallas_call(
        functools.partial(kernel, n),
        out_shape=(
            pltpu.VMEM((tok_rows, width), BF16),
            pltpu.VMEM((1, 128), F32),
        ),
        in_specs=[anywhere] * 7,
        out_specs=(pl.BlockSpec(memory_space=pltpu.VMEM),) * 2,
        scratch_shapes=[
            pltpu.VMEM((tok_rows, width), BF16),
            pltpu.VMEM((EXPERTS, width), BF16),
            pltpu.SMEM((2, tok_rows), jnp.int32),
            pltpu.SMEM((2, tok_rows), jnp.int32),
            pltpu.VMEM((W_SLOTS, k_rows, hidden), BF16),
            pltpu.VMEM((W_SLOTS, k_rows, hidden), BF16),
            pltpu.VMEM((MAIN_PARTS, hidden, d_cols), BF16),
            pltpu.VMEM((EXPERTS, CAP, width), BF16),
            pltpu.VMEM((n, CAP, width), BF16),
            pltpu.VMEM((n * CAP, hidden), F32),
            pltpu.VMEM((n * CAP, hidden), F32),
            pltpu.VMEM((n * CAP, hidden), BF16),
            pltpu.VMEM((2, chips * CAP, width), BF16),
            pltpu.VMEM((chips * CAP, width), BF16),
            pltpu.VMEM((chips, CAP, width), BF16),
            pltpu.VMEM((chips, CAP, width), BF16),
            pltpu.VMEM((TAIL_PARTS, n, CAP, d_cols // TAIL_PARTS), BF16),
            pltpu.VMEM((TAIL_PARTS, n, CAP, d_cols // TAIL_PARTS), BF16),
            pltpu.VMEM((tok_rows, 128), F32),
            pltpu.VMEM((8, 128), F32),
            pltpu.VMEM((chips, 8, 128), F32),
            pltpu.VMEM((2, 8, 128), F32),
            dma((W_SLOTS,)),
            dma((W_SLOTS,)),
            dma((MAIN_PARTS + TAIL_PARTS,)),
            dma((K_STEPS,)),
            dma((K_STEPS,)),
            dma((K_STEPS,)),
            dma((K_STEPS,)),
            dma((MAIN_PARTS,)),
            dma((MAIN_PARTS,)),
            dma((MAIN_PARTS,)),
            dma((MAIN_PARTS,)),
            dma((TAIL_PARTS,)),
            dma((TAIL_PARTS,)),
            dma((2,)),
            dma((2,)),
            dma((4,)),
        ],
        compiler_params=pltpu.CompilerParams(
            collective_id=0, has_side_effects=True, vmem_limit_bytes=66_800_000
        ),
    )(
        tokens,
        router_weight.T,
        expert_ids.T,
        slots.T,
        gate_weight,
        up_weight,
        down_weight,
    )
    inside = pl.BlockSpec(memory_space=pltpu.VMEM)
    mixed_rows, balance = pl.pallas_call(
        store,
        out_shape=(
            jax.ShapeDtypeStruct((tok_rows, width), BF16),
            jax.ShapeDtypeStruct((1, 128), F32),
        ),
        in_specs=[inside, inside],
        out_specs=(anywhere, anywhere),
        scratch_shapes=[dma((2,))],
        compiler_params=pltpu.CompilerParams(has_side_effects=True),
    )(
        pltpu.with_memory_space_constraint(mixed_rows, pltpu.VMEM),
        pltpu.with_memory_space_constraint(balance, pltpu.VMEM),
    )
    return mixed_rows, balance[0, :1]


def solution(mesh):
    in_specs = (
        P(("groups", "expert"), None),
        P("groups", None),
        P(("groups", "expert"), None),
        P(("groups", "expert"), None),
        P(None, "expert"),
        P(None, "expert"),
        P("expert", None),
    )
    out_specs = (P(("groups", "expert"), None), P("groups"))
    return jax.shard_map(
        functools.partial(local, mesh.shape["expert"]),
        mesh=mesh,
        in_specs=in_specs,
        out_specs=out_specs,
        check_vma=False,
    )
```

```python
import functools

import jax
import jax.numpy as jnp
from jax import lax
from jax.experimental import pallas as pl
from jax.experimental.pallas import tpu as pltpu
from jax.sharding import PartitionSpec as P

EXPERTS = 4
CAP = 2
MESH = pl.DeviceIdType.MESH
F32 = jnp.float32
BF16 = jnp.bfloat16

K_STEPS = 6
W_SLOTS = 5
D_PARTS = 6
MAIN_PARTS = 5
TAIL_PARTS = 2


def each(low, high, body):
    if high - low <= 16:
        for index in range(low, high):
            body(index)
    else:

        def step(index, carry):
            body(index)
            return carry

        lax.fori_loop(low, high, step, 0)


def kernel(
    n,
    tok_hbm,
    rw_hbm,
    ids_hbm,
    slots_hbm,
    gate_hbm,
    up_hbm,
    down_hbm,
    out_ref,
    bal_ref,
    tok_ref,
    rw_ref,
    ids_ref,
    slots_ref,
    gate_buf,
    up_buf,
    down_buf,
    send_x,
    x_buf,
    acc_g,
    acc_u,
    hid,
    part,
    pair,
    summed,
    back,
    tail_out,
    tail,
    weights,
    stat_own,
    stat_in,
    stat_pair,
    gate_sem,
    up_sem,
    down_sem,
    send_sem,
    xr_sem,
    fr_sem,
    pr_sem,
    br_sem,
    tr_sem,
    sr_sem,
    in_sem,
):
    me = lax.axis_index("expert")
    core = lax.rem(me, 2)
    chip = me // 2
    chips = n // 2
    per_expert = chips // EXPERTS
    partner = me + 1 - 2 * core
    tok_rows, width = tok_ref.shape
    k_rows = width // K_STEPS
    d_cols = width // D_PARTS
    t_cols = d_cols // TAIL_PARTS
    t_base = MAIN_PARTS * d_cols

    def chip_at(offset):
        return lax.rem(chip + offset, chips)

    def same_core(offset):
        return {"expert": chip_at(offset) * 2 + core}

    def weight_copy(k, source, target, sem):
        slot = lax.rem(k, W_SLOTS)
        rows = pl.ds(k * k_rows, k_rows)
        return pltpu.make_async_copy(source.at[rows], target.at[slot], sem.at[slot])

    def gate_copy(k):
        return weight_copy(k, gate_hbm, gate_buf, gate_sem)

    def up_copy(k):
        return weight_copy(k, up_hbm, up_buf, up_sem)

    def down_copy(j):
        cols = pl.ds(pl.multiple_of(j * d_cols, 128), d_cols)
        return pltpu.make_async_copy(down_hbm.at[:, cols], down_buf.at[j], down_sem.at[j])

    def tail_copy(t):
        cols = pl.ds(t_base + t * t_cols, t_cols)
        return pltpu.make_async_copy(
            down_hbm.at[:, cols],
            down_buf.at[0, :, pl.ds(t * t_cols, t_cols)],
            down_sem.at[MAIN_PARTS + t],
        )

    inputs = [
        pltpu.make_async_copy(source, target, in_sem.at[i])
        for i, (source, target) in enumerate(
            (
                (tok_hbm, tok_ref),
                (ids_hbm, ids_ref),
                (slots_hbm, slots_ref),
                (rw_hbm, rw_ref),
            )
        )
    ]
    for copy in inputs:
        copy.start()
    gate_copy(0).start()
    barrier = pltpu.get_barrier_semaphore()
    each(
        1,
        n,
        lambda o: pl.semaphore_signal(
            barrier, inc=1, device_id={"expert": lax.rem(me + o, n)}, device_id_type=MESH
        ),
    )

    for copy in inputs:
        copy.wait()
    up_copy(0).start()
    for k in range(1, W_SLOTS):
        gate_copy(k).start()
        up_copy(k).start()

    tok = tok_ref[...].astype(F32)
    ids = [[ids_ref[k, t] for k in range(2)] for t in range(tok_rows)]
    cells = [
        [
            jnp.where(slots_ref[k, t] < CAP, ids_ref[k, t] * CAP + slots_ref[k, t], -1)
            for k in range(2)
        ]
        for t in range(tok_rows)
    ]
    slot_of = lax.broadcasted_iota(jnp.int32, (CAP, width), 0)
    for e in range(EXPERTS):
        rows = jnp.zeros((CAP, width), F32)
        for t in range(tok_rows):
            for k in range(2):
                hit = slot_of + e * CAP == cells[t][k]
                rows = jnp.where(hit, jnp.broadcast_to(tok[t : t + 1], (CAP, width)), rows)
        send_x[e] = rows.astype(BF16)

    pl.semaphore_wait(barrier, n - 1)

    def k_cols_of(a):
        return pl.ds(pl.multiple_of(a * k_rows, 128), k_rows)

    def x_send(a, offset):
        return pltpu.make_async_remote_copy(
            src_ref=send_x.at[chip_at(offset) // per_expert, :, k_cols_of(a)],
            dst_ref=x_buf.at[core * chips + chip, :, k_cols_of(a)],
            send_sem=send_sem.at[0],
            recv_sem=xr_sem.at[a],
            device_id=same_core(offset),
            device_id_type=MESH,
        )

    def x_own(a):
        return pltpu.make_async_copy(
            send_x.at[chip // per_expert, :, k_cols_of(a)],
            x_buf.at[core * chips + chip, :, k_cols_of(a)],
            xr_sem.at[a],
        )

    def x_wait(a):
        half = x_buf.at[pl.ds(core * chips, chips), :, k_cols_of(a)]
        pltpu.make_async_copy(half, half, xr_sem.at[a]).wait()

    def x_forward(a):
        half = x_buf.at[pl.ds(core * chips, chips), :, k_cols_of(a)]
        return pltpu.make_async_remote_copy(
            src_ref=half,
            dst_ref=half,
            send_sem=send_sem.at[0],
            recv_sem=fr_sem.at[a],
            device_id={"expert": partner},
            device_id_type=MESH,
        )

    for a in range(K_STEPS):
        each(1, chips, lambda o, a=a: x_send(a, o).start())
        x_own(a).start()

    lane = lax.broadcasted_iota(jnp.int32, (tok_rows, 128), 1)
    row = lax.broadcasted_iota(jnp.int32, (tok_rows, 128), 0)
    logits = jnp.zeros((tok_rows, 128), F32)
    for e in range(EXPERTS):
        dots = jnp.sum(tok * rw_ref[e : e + 1, :].astype(F32), axis=1, keepdims=True)
        logits = jnp.where(lane == e, dots, logits)
    real = lane < EXPERTS
    top = jnp.max(jnp.where(real, logits, -jnp.inf), axis=1, keepdims=True)
    raised = jnp.where(real, jnp.exp(jnp.where(real, logits - top, 0.0)), 0.0)
    probs = raised / jnp.sum(raised, axis=1, keepdims=True)

    def column(values):
        result = jnp.zeros((tok_rows, 128), jnp.int32)
        for t in range(tok_rows):
            result = jnp.where(row == t, values[t], result)
        return result

    chosen = []
    for k in range(2):
        named = lane == column([ids[t][k] for t in range(tok_rows)])
        chosen.append(jnp.sum(jnp.where(named, logits, 0.0), axis=1, keepdims=True))
    top_two = jnp.maximum(chosen[0], chosen[1])
    lifted = [jnp.exp(value - top_two) for value in chosen]
    mix = jnp.zeros((tok_rows, 128), F32)
    for k in range(2):
        cell = column([cells[t][k] for t in range(tok_rows)])
        gate = lifted[k] / (lifted[0] + lifted[1])
        mix = mix + jnp.where(lane == cell, gate, 0.0)
    weights[...] = mix
    counts = jnp.zeros((tok_rows, 128), F32)
    for t in range(tok_rows):
        for k in range(2):
            counts = counts + jnp.where(lane == ids[t][k], 1.0, 0.0)
    stat_own[...] = jnp.zeros((8, 128), F32)
    stat_own[0:1] = counts[0:1]
    stat_own[1:2] = jnp.sum(probs, axis=0, keepdims=True)

    def stat_send(offset):
        return pltpu.make_async_remote_copy(
            src_ref=stat_own,
            dst_ref=stat_in.at[chip],
            send_sem=send_sem.at[0],
            recv_sem=sr_sem.at[0],
            device_id=same_core(offset),
            device_id_type=MESH,
        )

    def stat_swap():
        return pltpu.make_async_remote_copy(
            src_ref=stat_pair.at[0],
            dst_ref=stat_pair.at[1],
            send_sem=send_sem.at[0],
            recv_sem=sr_sem.at[1],
            device_id={"expert": partner},
            device_id_type=MESH,
        )

    each(1, chips, lambda o: stat_send(o).start())
    stat_mine = pltpu.make_async_copy(stat_own, stat_in.at[chip], sr_sem.at[0])
    stat_mine.start()

    acc_g[...] = jnp.zeros(acc_g.shape, F32)
    acc_u[...] = jnp.zeros(acc_u.shape, F32)

    x_wait(0)
    x_forward(0).start()

    def k_step(k, carry):
        @pl.when(k + 1 < K_STEPS)
        def _():
            x_wait(k + 1)
            x_forward(k + 1).start()

        x_forward(k).wait_recv()
        slot = lax.rem(k, W_SLOTS)
        cols = pl.ds(pl.multiple_of(k * k_rows, 128), k_rows)
        x = x_buf[:, :, cols].reshape(n * CAP, k_rows)
        gate_copy(k).wait()
        acc_g[...] += jnp.dot(x, gate_buf[slot], preferred_element_type=F32)
        up_copy(k).wait()
        acc_u[...] += jnp.dot(x, up_buf[slot], preferred_element_type=F32)

        @pl.when(k + W_SLOTS < K_STEPS)
        def _():
            gate_copy(k + W_SLOTS).start()
            up_copy(k + W_SLOTS).start()

        @pl.when((k >= 1) & (k <= MAIN_PARTS))
        def _():
            down_copy(k - 1).start()

        return carry

    lax.fori_loop(0, K_STEPS, k_step, 0)

    hid[...] = (jax.nn.silu(acc_g[...]) * acc_u[...]).astype(BF16)

    pltpu.make_async_copy(stat_in, stat_in, sr_sem.at[0]).wait()
    stat_pair[0] = jnp.sum(stat_in[...], axis=0)
    stat_swap().start()

    def d_cols_of(j):
        return pl.ds(pl.multiple_of(j * d_cols, 128), d_cols)

    def pair_send(j):
        return pltpu.make_async_remote_copy(
            src_ref=part.at[1 - core, :, d_cols_of(j)],
            dst_ref=pair.at[:, d_cols_of(j)],
            send_sem=send_sem.at[0],
            recv_sem=pr_sem.at[j],
            device_id={"expert": partner},
            device_id_type=MESH,
        )

    def back_send(j, offset):
        return pltpu.make_async_remote_copy(
            src_ref=summed.at[chip_at(offset), :, d_cols_of(j)],
            dst_ref=back.at[chip, :, d_cols_of(j)],
            send_sem=send_sem.at[0],
            recv_sem=br_sem.at[j],
            device_id=same_core(offset),
            device_id_type=MESH,
        )

    def back_own(j):
        return pltpu.make_async_copy(
            summed.at[chip, :, d_cols_of(j)], back.at[chip, :, d_cols_of(j)], br_sem.at[j]
        )

    def add_pair(j):
        pair_send(j).wait_recv()
        mine = part[core, :, d_cols_of(j)].astype(F32)
        both = (mine + pair[:, d_cols_of(j)].astype(F32)).astype(BF16)
        summed[:, :, d_cols_of(j)] = both.reshape(chips, CAP, d_cols)
        each(1, chips, lambda o: back_send(j, o).start())
        back_own(j).start()

    def d_step(j, carry):
        down_copy(j).wait()
        value = jnp.dot(hid[...], down_buf[j], preferred_element_type=F32)
        part[:, :, d_cols_of(j)] = value.astype(BF16).reshape(2, chips * CAP, d_cols)
        pair_send(j).start()

        @pl.when(j == 0)
        def _():
            for t in range(TAIL_PARTS):
                tail_copy(t).start()

        @pl.when(j > 0)
        def _():
            add_pair(j - 1)

        return carry

    def device_at(offset):
        return lax.rem(me + offset, n)

    def row_of(device):
        return lax.rem(device, 2) * chips + device // 2

    def tail_cols(t):
        return pl.ds(t_base + t * t_cols, t_cols)

    def tail_send(t, offset):
        return pltpu.make_async_remote_copy(
            src_ref=tail_out.at[t, row_of(device_at(offset))],
            dst_ref=tail.at[t, me],
            send_sem=send_sem.at[0],
            recv_sem=tr_sem.at[t],
            device_id={"expert": device_at(offset)},
            device_id_type=MESH,
        )

    def tail_own(t):
        return pltpu.make_async_copy(
            tail_out.at[t, row_of(me)], tail.at[t, me], tr_sem.at[t]
        )

    lax.fori_loop(0, MAIN_PARTS, d_step, 0)
    for t in range(TAIL_PARTS):
        tail_copy(t).wait()
        weight = down_buf[0, :, t * t_cols : (t + 1) * t_cols]
        value = jnp.dot(hid[...], weight, preferred_element_type=F32)
        if t == TAIL_PARTS - 1:
            add_pair(MAIN_PARTS - 1)
        tail_out[t] = value.astype(BF16).reshape(n, CAP, t_cols)
        each(1, n, lambda o, t=t: tail_send(t, o).start())
        tail_own(t).start()

    stat_swap().wait_recv()
    total = stat_pair[0] + stat_pair[1]
    tokens_in_all = float(tok_rows * n)
    terms = (total[0:1] / (2.0 * tokens_in_all)) * (total[1:2] / tokens_in_all)
    bal_ref[...] = jnp.broadcast_to(EXPERTS * jnp.sum(terms, axis=1, keepdims=True), (1, 128))
    stat_swap().wait_send()
    each(1, chips, lambda o: stat_send(o).wait_send())
    for a in range(K_STEPS):
        each(1, chips, lambda o, a=a: x_send(a, o).wait_send())
        x_forward(a).wait_send()

    mix_of = [weights[:, c : c + 1] for c in range(EXPERTS * CAP)]

    def mix_rows(blocks, cols, per_block):
        count = per_expert * per_block
        mixed = jnp.zeros((tok_rows, cols.size), F32)
        for e in range(EXPERTS):
            value = jnp.sum(blocks[e * count : (e + 1) * count].astype(F32), axis=0)
            for c in range(CAP):
                mixed = mixed + mix_of[e * CAP + c] * value[c : c + 1]
        out_ref[:, cols] = mixed.astype(BF16)

    for j in range(MAIN_PARTS):
        pair_send(j).wait_send()
        each(1, chips, lambda o, j=j: back_send(j, o).wait_send())
        cols = pl.ds(j * d_cols, d_cols)
        whole = back.at[:, :, cols]
        pltpu.make_async_copy(whole, whole, br_sem.at[j]).wait()
        mix_rows(back[:, :, cols], cols, 1)
    for t in range(TAIL_PARTS):
        each(1, n, lambda o, t=t: tail_send(t, o).wait_send())
    for t in range(TAIL_PARTS):
        pltpu.make_async_copy(tail.at[t], tail.at[t], tr_sem.at[t]).wait()
        mix_rows(tail[t], tail_cols(t), 2)


def store(mixed_ref, bal_ref, mixed_hbm, bal_hbm, sem):
    copies = (
        pltpu.make_async_copy(mixed_ref, mixed_hbm, sem.at[0]),
        pltpu.make_async_copy(bal_ref, bal_hbm, sem.at[1]),
    )
    for copy in copies:
        copy.start()
    for copy in copies:
        copy.wait()


def local(n, tokens, router_weight, expert_ids, slots, gate_weight, up_weight, down_weight):
    tok_rows, width = tokens.shape
    hidden = gate_weight.shape[1]
    chips = n // 2
    k_rows, d_cols = width // K_STEPS, width // D_PARTS
    anywhere = pl.BlockSpec(memory_space=pl.ANY)
    dma = pltpu.SemaphoreType.DMA
    mixed_rows, balance = pl.pallas_call(
        functools.partial(kernel, n),
        out_shape=(
            pltpu.VMEM((tok_rows, width), BF16),
            pltpu.VMEM((1, 128), F32),
        ),
        in_specs=[anywhere] * 7,
        out_specs=(pl.BlockSpec(memory_space=pltpu.VMEM),) * 2,
        scratch_shapes=[
            pltpu.VMEM((tok_rows, width), BF16),
            pltpu.VMEM((EXPERTS, width), BF16),
            pltpu.SMEM((2, tok_rows), jnp.int32),
            pltpu.SMEM((2, tok_rows), jnp.int32),
            pltpu.VMEM((W_SLOTS, k_rows, hidden), BF16),
            pltpu.VMEM((W_SLOTS, k_rows, hidden), BF16),
            pltpu.VMEM((MAIN_PARTS, hidden, d_cols), BF16),
            pltpu.VMEM((EXPERTS, CAP, width), BF16),
            pltpu.VMEM((n, CAP, width), BF16),
            pltpu.VMEM((n * CAP, hidden), F32),
            pltpu.VMEM((n * CAP, hidden), F32),
            pltpu.VMEM((n * CAP, hidden), BF16),
            pltpu.VMEM((2, chips * CAP, width), BF16),
            pltpu.VMEM((chips * CAP, width), BF16),
            pltpu.VMEM((chips, CAP, width), BF16),
            pltpu.VMEM((chips, CAP, width), BF16),
            pltpu.VMEM((TAIL_PARTS, n, CAP, d_cols // TAIL_PARTS), BF16),
            pltpu.VMEM((TAIL_PARTS, n, CAP, d_cols // TAIL_PARTS), BF16),
            pltpu.VMEM((tok_rows, 128), F32),
            pltpu.VMEM((8, 128), F32),
            pltpu.VMEM((chips, 8, 128), F32),
            pltpu.VMEM((2, 8, 128), F32),
            dma((W_SLOTS,)),
            dma((W_SLOTS,)),
            dma((MAIN_PARTS + TAIL_PARTS,)),
            dma((1,)),
            dma((K_STEPS,)),
            dma((K_STEPS,)),
            dma((MAIN_PARTS,)),
            dma((MAIN_PARTS,)),
            dma((TAIL_PARTS,)),
            dma((2,)),
            dma((4,)),
        ],
        compiler_params=pltpu.CompilerParams(
            collective_id=0, has_side_effects=True, vmem_limit_bytes=66_800_000
        ),
    )(
        tokens,
        router_weight.T,
        expert_ids.T,
        slots.T,
        gate_weight,
        up_weight,
        down_weight,
    )
    inside = pl.BlockSpec(memory_space=pltpu.VMEM)
    mixed_rows, balance = pl.pallas_call(
        store,
        out_shape=(
            jax.ShapeDtypeStruct((tok_rows, width), BF16),
            jax.ShapeDtypeStruct((1, 128), F32),
        ),
        in_specs=[inside, inside],
        out_specs=(anywhere, anywhere),
        scratch_shapes=[dma((2,))],
        compiler_params=pltpu.CompilerParams(has_side_effects=True),
    )(
        pltpu.with_memory_space_constraint(mixed_rows, pltpu.VMEM),
        pltpu.with_memory_space_constraint(balance, pltpu.VMEM),
    )
    return mixed_rows, balance[0, :1]


def solution(mesh):
    in_specs = (
        P(("groups", "expert"), None),
        P("groups", None),
        P(("groups", "expert"), None),
        P(("groups", "expert"), None),
        P(None, "expert"),
        P(None, "expert"),
        P("expert", None),
    )
    out_specs = (P(("groups", "expert"), None), P("groups"))
    return jax.shard_map(
        functools.partial(local, mesh.shape["expert"]),
        mesh=mesh,
        in_specs=in_specs,
        out_specs=out_specs,
        check_vma=False,
    )
```
